256 devices in a mesh: snap: 4 (over z_hi), param: 64 (over z_lo, x, y, core).
Axes of the slice: x: 4, y: 4, z: 8 (z_hi: 4, z_lo: 2; z = z_hi * 2 + z_lo), core: 2. Of those that a mesh axis runs over, the one named last changes fastest.
Arguments:
- snapshots: bfloat16 [256, 4096, 1024], P('snap', 'param'), as said below
- coeffs: float32 [16, 256], P(None, 'snap'), may hold values from -0.375 to 0.375
Outputs:
- averages: float32 [16, 4096, 1024], P(None, 'param', 'snap')
- width_norms: float32 [16], replicated
The draws below stay inside these ranges and needn't reach their ends.
Inputs may be any that keep to these rules, and one draw needn't show every extreme that they name: `snapshots`: stored snapshot weights, finite.
All inputs are finite; a program needn't handle non-finite values.
Results may differ from the reference program's by a relative error of at most 0.0003.
Values may be sent and summed in bfloat16 or wider, within the bound.
No kernel may reach another device: no remote copies, remote signals or barrier semaphores. Data moves between devices by JAX's collectives and lax.ppermute only.
A program may use at most 64 MiB of HBM per device.

```python
import math
import jax
import jax.numpy as jnp
from jax import lax

WIDTHS = 16
COLS = 1024
NSNAP = 256
ROWS = 4096


def draw_snapshots(key, part):
    key_rows = jax.random.fold_in(key, 11)
    key_cols = jax.random.fold_in(key, 12)
    key_base = jax.random.fold_in(key, 13)
    row_index = jnp.arange(ROWS, dtype=jnp.float32)
    row_scale = 3.0 ** (row_index / ROWS) * 10.0 ** jax.random.uniform(key_rows, (ROWS,), jnp.float32)
    col_scale = 10.0 ** jax.random.uniform(key_cols, (COLS,), jnp.float32)
    base = jax.random.normal(key_base, (NSNAP, ROWS, COLS), jnp.float32)
    values = base * row_scale[None, :, None] * col_scale[None, None, :] / 10.0
    return values.astype(jnp.bfloat16)


def block_scale(key, shape, shards, least, largest):
    loudness, own = 1.0, jax.random.fold_in(key, 6)
    for dim, blocks in shards:
        draws = jnp.exp(jax.random.uniform(jax.random.fold_in(own, dim), (blocks,), jnp.float32, least / len(shards), largest / len(shards)))
        loudness = loudness * jnp.repeat(draws, shape[dim] // blocks).reshape([-1 if axis == dim else 1 for axis in range(len(shape))])
    return loudness


def gaussian(rng, extent, deviation, most, cuts=(), kind=jnp.bfloat16):
    values = jax.random.normal(rng, extent, jnp.float32) * deviation
    if len(cuts) > 0:
        values = block_scale(rng, extent, cuts, -0.22, 0.18) * values
    return jnp.clip(values, min=-most, max=most).astype(kind)


def setup_inputs(seed: int = 0) -> dict:
    splits = jax.random.split(jax.random.key(seed), 3)
    snapshots = draw_snapshots(jax.random.fold_in(splits[2], 71), 0)
    coeffs = gaussian(splits[1], (WIDTHS, NSNAP), NSNAP ** -0.5, 0.375, ((1, 4),), jnp.float32)
    return dict(snapshots=snapshots, coeffs=coeffs)


def reference(snapshots, coeffs):
    block_rows = math.gcd(ROWS, 256)
    block_count = ROWS // block_rows

    def one_block(block_index):
        start = (block_index * block_rows).astype(jnp.int32)
        piece = lax.dynamic_slice_in_dim(snapshots, start, block_rows, 1).astype(jnp.float32)
        flat = piece.reshape(NSNAP, block_rows * COLS)
        product = jnp.dot(coeffs.astype(jnp.float32), flat, precision=lax.Precision.HIGHEST, preferred_element_type=jnp.float32)
        return product.reshape(WIDTHS, block_rows, COLS)
    stacked = lax.map(one_block, jnp.arange(block_count, dtype=jnp.int32))
    averages = jnp.transpose(stacked, (1, 0, 2, 3)).reshape(WIDTHS, ROWS, COLS)
    squares = lax.optimization_barrier(jnp.sum(averages * averages, axis=(1, 2)))
    width_norms = jnp.sqrt(squares / jnp.float32(ROWS * COLS))
    return (averages, width_norms)
```

```python
import functools

import jax
import jax.numpy as jnp
from jax import lax
from jax.experimental import pallas as pl
from jax.experimental.pallas import tpu as pltpu
from jax.sharding import PartitionSpec as P

GROUP = 16
HALF = 128
CHUNK = 256
PARTS = (32, 32)

SPAN = 250.0
LN2 = 0.6931471805599453
PRE = 2.0**-8


def column_scale(values):
    top = jnp.max(jnp.abs(values), axis=0, keepdims=True)
    scale = jnp.clip(top * 1.0079, 2.0**-116, 3.38e38)
    return scale.astype(jnp.bfloat16).astype(jnp.float32)


def encode(values, scale):
    inverse = 1.0 / (scale * PRE)
    level = jnp.abs(values) * inverse * (SPAN * LN2 * PRE) - (SPAN / 2 * LN2)
    code = jnp.exp(level)
    return jnp.where(values < 0, -code, code).astype(jnp.bfloat16)


def decode(code, scale):
    code = code.astype(jnp.float32)
    level = jnp.log(jnp.abs(code)) + (SPAN / 2 * LN2)
    return jnp.where(code < 0, -level, level) * (scale * (1.0 / (SPAN * LN2)))


def partial_kernel(start, rows, x_ref, c_ref, up_ref, down_ref, own_ref, fwd_up_ref, fwd_down_ref, xbuf, wide, hold, scales, sems):
    widths, snaps = c_ref.shape
    blocks = rows // GROUP
    depth = snaps * GROUP
    me = lax.axis_index("snap")
    copies = []
    for block in range(blocks):
        for j in range(4):
            column = pl.multiple_of(lax.rem(me + j, 4) * CHUNK, CHUNK)
            copies.append(
                pltpu.make_async_copy(
                    x_ref.at[:, pl.ds(start + block * GROUP, GROUP), pl.ds(column, CHUNK)],
                    xbuf.at[block, :, :, pl.ds(j * CHUNK, CHUNK)],
                    sems.at[block, j],
                )
            )
            copies[-1].start()

    coeffs = c_ref[...]
    high = coeffs.astype(jnp.bfloat16)
    low = (coeffs - high.astype(jnp.float32)).astype(jnp.bfloat16)
    spread = (
        lax.shift_right_logical(lax.broadcasted_iota(jnp.int32, (snaps, depth), 1), 4)
        == lax.broadcasted_iota(jnp.int32, (snaps, depth), 0)
    ).astype(jnp.float32).astype(jnp.bfloat16)
    keep = (lax.broadcasted_iota(jnp.int32, (GROUP, depth), 1) & (GROUP - 1)) == lax.broadcasted_iota(
        jnp.int32, (GROUP, depth), 0
    )
    for part, piece in enumerate((high, low)):
        across = jnp.dot(piece, spread, preferred_element_type=jnp.float32)
        for w in range(widths):
            row = (part * widths + w) * GROUP
            wide[row : row + GROUP, :] = jnp.where(keep, across[w : w + 1, :], 0.0).astype(jnp.bfloat16)

    for block in range(blocks):
        r = slice(block * GROUP, (block + 1) * GROUP)
        for j in range(4):
            copies[block * 4 + j].wait()
            flat = xbuf[block, :, :, j * CHUNK : (j + 1) * CHUNK].reshape(depth, CHUNK)
            both = jnp.dot(wide[...], flat, preferred_element_type=jnp.float32)
            value = (both[: widths * GROUP] + both[widths * GROUP :]).reshape(widths, GROUP, CHUNK)
            if j == 0:
                own_ref[:, r, :] = value
            elif j == 1:
                fwd_up_ref[:, r, :] = value[:, :, :HALF]
                hold[:, r, HALF : 2 * HALF] = value[:, :, HALF:]
            elif j == 2:
                hold[:, r, :HALF] = value[:, :, :HALF]
                hold[:, r, 2 * HALF : 3 * HALF] = value[:, :, HALF:]
            else:
                hold[:, r, 3 * HALF :] = value[:, :, :HALF]
                fwd_down_ref[:, r, :] = value[:, :, HALF:]

    for w in range(widths):
        value = hold[w]
        scale = column_scale(value)
        scales[w : w + 1, :] = scale
        code = encode(value, scale)
        up_ref[w * rows : (w + 1) * rows, :] = code[:, :CHUNK]
        down_ref[w * rows : (w + 1) * rows, :] = code[:, CHUNK:]
    packed = scales[...].astype(jnp.bfloat16)
    up_ref[widths * rows :, :] = packed[:, :CHUNK]
    down_ref[widths * rows :, :] = packed[:, CHUNK:]


def relay_kernel(rows, prev_ref, next_ref, own_ref, fwd_up_ref, fwd_down_ref, up_ref, down_ref, sum_ref, scales):
    widths = own_ref.shape[0]
    prev_scale = prev_ref[widths * rows :, :].astype(jnp.float32)
    next_scale = next_ref[widths * rows :, :].astype(jnp.float32)
    for w in range(widths):
        r = slice(w * rows, (w + 1) * rows)
        got_prev = decode(prev_ref[r, :], prev_scale[w : w + 1, :])
        got_next = decode(next_ref[r, :], next_scale[w : w + 1, :])
        up = fwd_up_ref[w] + got_prev[:, :HALF]
        down = fwd_down_ref[w] + got_next[:, :HALF]
        up_scale = column_scale(up)
        down_scale = column_scale(down)
        scales[w : w + 1, :HALF] = up_scale
        scales[w : w + 1, HALF:] = down_scale
        up_ref[r, :] = encode(up, up_scale)
        down_ref[r, :] = encode(down, down_scale)
        sum_ref[w, :, :HALF] = own_ref[w, :, :HALF] + got_next[:, HALF:]
        sum_ref[w, :, HALF:] = own_ref[w, :, HALF:] + got_prev[:, HALF:]
    packed = scales[...].astype(jnp.bfloat16)
    up_ref[widths * rows :, :] = packed[:, :HALF]
    down_ref[widths * rows :, :] = packed[:, HALF:]


def final_kernel(rows, devices, prev_ref, next_ref, sum_ref, before_ref, out_ref, squares_ref):
    widths = sum_ref.shape[0]
    prev_scale = prev_ref[widths * rows :, :].astype(jnp.float32)
    next_scale = next_ref[widths * rows :, :].astype(jnp.float32)
    for w in range(widths):
        r = slice(w * rows, (w + 1) * rows)
        left = sum_ref[w, :, :HALF] + decode(prev_ref[r, :], prev_scale[w : w + 1, :])
        right = sum_ref[w, :, HALF:] + decode(next_ref[r, :], next_scale[w : w + 1, :])
        out_ref[w, :, :HALF] = left
        out_ref[w, :, HALF:] = right
        squares_ref[w : w + 1, :] = before_ref[w : w + 1, :] + jnp.sum(left * left + right * right, axis=0, keepdims=True)


def vmem():
    return pl.BlockSpec(memory_space=pltpu.VMEM)


def partial_sums(snapshots, coeffs, start, rows):
    widths, snaps = coeffs.shape
    shape = jax.ShapeDtypeStruct
    tall = widths * rows + widths
    blocks = rows // GROUP
    return pl.pallas_call(
        functools.partial(partial_kernel, start, rows),
        in_specs=[pl.BlockSpec(memory_space=pl.ANY), vmem()],
        out_specs=[vmem()] * 5,
        out_shape=[
            shape((tall, CHUNK), jnp.bfloat16),
            shape((tall, CHUNK), jnp.bfloat16),
            shape((widths, rows, CHUNK), jnp.float32),
            shape((widths, rows, HALF), jnp.float32),
            shape((widths, rows, HALF), jnp.float32),
        ],
        scratch_shapes=[
            pltpu.VMEM((blocks, snaps, GROUP, 4 * CHUNK), jnp.bfloat16),
            pltpu.VMEM((2 * widths * GROUP, snaps * GROUP), jnp.bfloat16),
            pltpu.VMEM((widths, rows, 4 * HALF), jnp.float32),
            pltpu.VMEM((widths, 4 * HALF), jnp.float32),
            pltpu.SemaphoreType.DMA((blocks, 4)),
        ],
        cost_estimate=pl.CostEstimate(flops=6_000_000_000, bytes_accessed=6_000_000, transcendentals=0),
        name="partial_sums",
    )(snapshots, coeffs)


def relay(rows, got_prev, got_next, own, fwd_up, fwd_down):
    widths = own.shape[0]
    shape = jax.ShapeDtypeStruct
    tall = widths * rows + widths
    return pl.pallas_call(
        functools.partial(relay_kernel, rows),
        in_specs=[vmem()] * 5,
        out_specs=[vmem()] * 3,
        out_shape=[
            shape((tall, HALF), jnp.bfloat16),
            shape((tall, HALF), jnp.bfloat16),
            shape(own.shape, jnp.float32),
        ],
        scratch_shapes=[pltpu.VMEM((widths, CHUNK), jnp.float32)],
        cost_estimate=pl.CostEstimate(flops=2_000_000_000, bytes_accessed=2_000_000, transcendentals=0),
        name="relay",
    )(got_prev, got_next, own, fwd_up, fwd_down)


def finish(rows, got_prev, got_next, summed, squares):
    widths = summed.shape[0]
    shape = jax.ShapeDtypeStruct
    return pl.pallas_call(
        functools.partial(final_kernel, rows, 0),
        in_specs=[vmem()] * 4,
        out_specs=[vmem()] * 2,
        out_shape=[shape(summed.shape, jnp.float32), shape((widths, HALF), jnp.float32)],
        cost_estimate=pl.CostEstimate(flops=1_000_000_000, bytes_accessed=2_000_000, transcendentals=0),
        name="finish",
    )(got_prev, got_next, summed, squares)


def on_device(snapshots, coeffs):
    axes = ("snap", "param")
    groups = lax.axis_size("snap")
    devices = lax.axis_size(axes)
    widths = coeffs.shape[0]
    up_pairs = [(i, (i + 1) % groups) for i in range(groups)]
    down_pairs = [(i, (i - 1) % groups) for i in range(groups)]

    starts = [sum(PARTS[:k]) for k in range(len(PARTS))]
    first = []
    for start, rows in zip(starts, PARTS):
        up, down, own, fwd_up, fwd_down = partial_sums(snapshots, coeffs, start, rows)
        got_prev = lax.ppermute(up, "snap", up_pairs)
        got_next = lax.ppermute(down, "snap", down_pairs)
        first.append((got_prev, got_next, own, fwd_up, fwd_down))
    second = []
    for rows, part in zip(PARTS, first):
        up, down, summed = relay(rows, *part)
        got_prev = lax.ppermute(up, "snap", up_pairs)
        got_next = lax.ppermute(down, "snap", down_pairs)
        second.append((got_prev, got_next, summed))
    squares = jnp.zeros((widths, HALF), jnp.float32)
    outs = []
    for rows, part in zip(PARTS, second):
        out, squares = finish(rows, *part, squares)
        outs.append(out)
    averages = jnp.concatenate(outs, axis=1)
    mine = jnp.broadcast_to(jnp.sum(squares, axis=1)[None, :], (devices, widths))
    theirs = lax.all_to_all(mine, axes, 0, 0, tiled=True)
    entries = averages.shape[1] * averages.shape[2] * devices
    width_norms = jnp.sqrt(jnp.sum(theirs, axis=0) / jnp.float32(entries))
    return (averages, width_norms)


def solution(mesh):
    return jax.shard_map(
        on_device,
        mesh=mesh,
        in_specs=(P("snap", "param", None), P(None, "snap")),
        out_specs=(P(None, "param", "snap"), P()),
        check_vma=False,
    )
```

```python
import functools

import jax
import jax.numpy as jnp
from jax import lax
from jax.experimental import pallas as pl
from jax.experimental.pallas import tpu as pltpu
from jax.sharding import PartitionSpec as P


GROUP = 8
BLOCK = 16
FLIGHT = 2
HALF = 128
CHUNK = 256
PARTS = (32, 32)

SPAN = 250.0
LN2 = 0.6931471805599453
PRE = 2.0**-8


def column_scale(values):
    top = jnp.max(jnp.abs(values), axis=0, keepdims=True)
    scale = jnp.clip(top * 1.0079, 2.0**-116, 3.38e38)
    return scale.astype(jnp.bfloat16).astype(jnp.float32)


def encode(values, scale):
    inverse = (SPAN * LN2 * PRE) / (scale * PRE)
    code = jnp.exp(jnp.abs(values) * inverse - (SPAN / 2 * LN2))
    return jnp.where(values < 0, -code, code).astype(jnp.bfloat16)


def decode(code, scale):
    code = code.astype(jnp.float32)
    level = jnp.log(jnp.abs(code)) + (SPAN / 2 * LN2)
    return jnp.where(code < 0, -level, level) * (scale * (1.0 / (SPAN * LN2)))


def fill_wide(c_ref, cbuf, sem, wide):
    widths, snaps = c_ref.shape
    depth = snaps * GROUP
    pltpu.make_async_copy(c_ref, cbuf, sem).wait()
    coeffs = cbuf[...]
    high = coeffs.astype(jnp.bfloat16)
    low = (coeffs - high.astype(jnp.float32)).astype(jnp.bfloat16)
    spread = (
        lax.shift_right_logical(lax.broadcasted_iota(jnp.int32, (snaps, depth), 1), 3)
        == lax.broadcasted_iota(jnp.int32, (snaps, depth), 0)
    ).astype(jnp.float32).astype(jnp.bfloat16)
    keep = (lax.broadcasted_iota(jnp.int32, (GROUP, depth), 1) & (GROUP - 1)) == lax.broadcasted_iota(
        jnp.int32, (GROUP, depth), 0
    )
    for part, piece in enumerate((high, low)):
        across = jnp.dot(piece, spread, preferred_element_type=jnp.float32)
        for w in range(widths):
            row = (part * widths + w) * GROUP
            wide[row : row + GROUP, :] = jnp.where(keep, across[w : w + 1, :], 0.0).astype(jnp.bfloat16)


def half_of(offset):
    return pl.multiple_of(lax.rem(2 * lax.axis_index("snap") + offset, 8) * HALF, HALF)


def multiply(x_ref, wide, start, offsets):
    depth = wide.shape[1]
    half = wide.shape[0] // 2
    halves = [x_ref[:, start : start + GROUP, pl.ds(half_of(offset), HALF)].reshape(depth, HALF) for offset in offsets]
    both = jnp.dot(wide[...], jnp.concatenate(halves, axis=1), preferred_element_type=jnp.float32)
    return (both[:half] + both[half:]).reshape(half // GROUP, GROUP, CHUNK)


def sent_kernel(start, rows, first, x_ref, c_ref, *refs):
    if first:
        up_ref, down_ref, x_out, wide, cbuf, csem, hold, scales, sems = refs
        pltpu.make_async_copy(c_ref, cbuf, csem).start()
    else:
        wide = c_ref
        up_ref, down_ref, x_out, hold, scales, sems = refs
    widths = wide.shape[0] // (2 * GROUP)
    blocks = rows // BLOCK
    copies = [
        pltpu.make_async_copy(
            x_ref.at[:, pl.ds(start + block * BLOCK, BLOCK), :],
            x_out.at[:, pl.ds(block * BLOCK, BLOCK), :],
            sems.at[block],
        )
        for block in range(blocks)
    ]
    for copy in copies[:FLIGHT]:
        copy.start()
    if first:
        fill_wide(c_ref, cbuf, csem, wide)
    for block in range(blocks):
        copies[block].wait()
        if block + FLIGHT < blocks:
            copies[block + FLIGHT].start()
        for at in range(block * BLOCK, (block + 1) * BLOCK, GROUP):
            hold[:, at : at + GROUP, :CHUNK] = multiply(x_out, wide, at, (4, 3))
            hold[:, at : at + GROUP, CHUNK:] = multiply(x_out, wide, at, (5, 6))
    for w in range(widths):
        value = hold[w]
        scale = column_scale(value)
        scales[w : w + 1, :] = scale
        code = encode(value, scale)
        up_ref[w * rows : (w + 1) * rows, :] = code[:, :CHUNK]
        down_ref[w * rows : (w + 1) * rows, :] = code[:, CHUNK:]
    packed = scales[...].astype(jnp.bfloat16)
    up_ref[widths * rows :, :] = packed[:, :CHUNK]
    down_ref[widths * rows :, :] = packed[:, CHUNK:]


def kept_kernel(wide, *refs):
    x_refs, (own_ref, fwd_up_ref, fwd_down_ref) = refs[:-3], refs[-3:]
    start = 0
    for x_ref in x_refs:
        for at in range(0, x_ref.shape[1], GROUP):
            r = slice(start + at, start + at + GROUP)
            own_ref[:, r, :] = multiply(x_ref, wide, at, (0, 1))
            value = multiply(x_ref, wide, at, (2, 7))
            fwd_up_ref[:, r, :] = value[:, :, :HALF]
            fwd_down_ref[:, r, :] = value[:, :, HALF:]
        start += x_ref.shape[1]


def relay_kernel(start, rows, prev_ref, next_ref, own_ref, fwd_up_ref, fwd_down_ref, up_ref, down_ref, sum_ref, scales):
    widths = own_ref.shape[0]
    t = slice(start, start + rows)
    prev_scale = prev_ref[widths * rows :, :].astype(jnp.float32)
    next_scale = next_ref[widths * rows :, :].astype(jnp.float32)
    for w in range(widths):
        r = slice(w * rows, (w + 1) * rows)
        got_prev = decode(prev_ref[r, :], prev_scale[w : w + 1, :])
        got_next = decode(next_ref[r, :], next_scale[w : w + 1, :])
        up = fwd_up_ref[w, t, :] + got_prev[:, :HALF]
        down = fwd_down_ref[w, t, :] + got_next[:, :HALF]
        up_scale = column_scale(up)
        down_scale = column_scale(down)
        scales[w : w + 1, :HALF] = up_scale
        scales[w : w + 1, HALF:] = down_scale
        up_ref[r, :] = encode(up, up_scale)
        down_ref[r, :] = encode(down, down_scale)
        sum_ref[w, :, :HALF] = own_ref[w, t, :HALF] + got_next[:, HALF:]
        sum_ref[w, :, HALF:] = own_ref[w, t, HALF:] + got_prev[:, HALF:]
    packed = scales[...].astype(jnp.bfloat16)
    up_ref[widths * rows :, :] = packed[:, :HALF]
    down_ref[widths * rows :, :] = packed[:, HALF:]


def final_kernel(start, rows, first, last, prev_ref, next_ref, sum_ref, *refs):
    refs = list(refs)
    before_ref = None if first else refs.pop(0)
    if not first:
        refs.pop(0)
    out_ref, squares_ref, block, total, sem = refs
    widths = sum_ref.shape[0]
    prev_scale = prev_ref[widths * rows :, :].astype(jnp.float32)
    next_scale = next_ref[widths * rows :, :].astype(jnp.float32)
    for w in range(widths):
        r = slice(w * rows, (w + 1) * rows)
        left = sum_ref[w, :, :HALF] + decode(prev_ref[r, :], prev_scale[w : w + 1, :])
        right = sum_ref[w, :, HALF:] + decode(next_ref[r, :], next_scale[w : w + 1, :])
        block[w, :, :HALF] = left
        block[w, :, HALF:] = right
        total[w : w + 1, :] = jnp.sum(left * left + right * right, axis=0, keepdims=True)
    copy = pltpu.make_async_copy(block, out_ref.at[:, pl.ds(start, rows), :], sem)
    copy.start()
    squares = total[...] if first else total[...] + before_ref[...]
    if last:
        squares = lax.dot_general(
            jnp.ones((squares_ref.shape[0], HALF), jnp.float32),
            squares,
            (((1,), (1,)), ((), ())),
            precision=lax.Precision.HIGHEST,
            preferred_element_type=jnp.float32,
        )
    squares_ref[...] = squares
    copy.wait()


def vmem():
    return pl.BlockSpec(memory_space=pltpu.VMEM)


def hbm():
    return pl.BlockSpec(memory_space=pl.ANY)


def held(array):
    return pltpu.with_memory_space_constraint(array, pltpu.VMEM)


def placed(array):
    return pltpu.with_memory_space_constraint(array, pltpu.HBM)


def cost(flops):
    return pl.CostEstimate(flops=flops, bytes_accessed=2_000_000, transcendentals=0)


def params(mib):
    return pltpu.CompilerParams(vmem_limit_bytes=mib * 2**20)


def sent_sums(snapshots, start, rows, coeffs=None, wide=None):
    first = wide is None
    snaps, _, columns = snapshots.shape
    widths = coeffs.shape[0] if first else wide.shape[0] // (2 * GROUP)
    tall = widths * rows + widths
    wide_shape = pltpu.VMEM((2 * widths * GROUP, snaps * GROUP), jnp.bfloat16)
    return pl.pallas_call(
        functools.partial(sent_kernel, start, rows, first),
        in_specs=[hbm(), hbm() if first else vmem()],
        out_specs=[vmem()] * (4 if first else 3),
        out_shape=[pltpu.VMEM((tall, CHUNK), jnp.bfloat16)] * 2
        + [pltpu.VMEM((snaps, rows, columns), jnp.bfloat16)]
        + [wide_shape] * first,
        scratch_shapes=[pltpu.VMEM((widths, snaps), jnp.float32), pltpu.SemaphoreType.DMA] * first
        + [
            pltpu.VMEM((widths, rows, 2 * CHUNK), jnp.float32),
            pltpu.VMEM((widths, 2 * CHUNK), jnp.float32),
            pltpu.SemaphoreType.DMA((rows // BLOCK,)),
        ],
        cost_estimate=cost(4_000_000_000),
        compiler_params=params(14),
        name="sent_sums",
    )(placed(snapshots), placed(coeffs) if first else held(wide))


def kept_sums(wide, parts):
    widths = wide.shape[0] // (2 * GROUP)
    rows = sum(part.shape[1] for part in parts)
    return pl.pallas_call(
        kept_kernel,
        in_specs=[vmem()] * (1 + len(parts)),
        out_specs=[vmem()] * 3,
        out_shape=[
            pltpu.VMEM((widths, rows, CHUNK), jnp.float32),
            pltpu.VMEM((widths, rows, HALF), jnp.float32),
            pltpu.VMEM((widths, rows, HALF), jnp.float32),
        ],
        cost_estimate=cost(6_000_000_000),
        compiler_params=params(16),
        name="kept_sums",
    )(held(wide), *[held(part) for part in parts])


def relay(start, rows, got_prev, got_next, own, fwd_up, fwd_down):
    widths = own.shape[0]
    tall = widths * rows + widths
    return pl.pallas_call(
        functools.partial(relay_kernel, start, rows),
        in_specs=[vmem()] * 5,
        out_specs=[vmem()] * 3,
        out_shape=[
            pltpu.VMEM((tall, HALF), jnp.bfloat16),
            pltpu.VMEM((tall, HALF), jnp.bfloat16),
            pltpu.VMEM((widths, rows, CHUNK), jnp.float32),
        ],
        scratch_shapes=[pltpu.VMEM((widths, CHUNK), jnp.float32)],
        cost_estimate=cost(2_000_000_000),
        compiler_params=params(4),
        name="relay",
    )(held(got_prev), held(got_next), held(own), held(fwd_up), held(fwd_down))


def finish(start, rows, total_rows, devices, last, got_prev, got_next, summed, squares, averages):
    widths = summed.shape[0]
    first = averages is None
    operands = [held(got_prev), held(got_next), held(summed)]
    specs = [vmem()] * 3
    if not first:
        operands += [held(squares), averages]
        specs += [vmem(), hbm()]
    return pl.pallas_call(
        functools.partial(final_kernel, start, rows, first, last),
        in_specs=specs,
        out_specs=[hbm(), vmem()],
        out_shape=[
            jax.ShapeDtypeStruct((widths, total_rows, CHUNK), jnp.float32),
            pltpu.VMEM((devices, widths) if last else (widths, HALF), jnp.float32),
        ],
        input_output_aliases={} if first else {4: 0},
        scratch_shapes=[
            pltpu.VMEM((widths, rows, CHUNK), jnp.float32),
            pltpu.VMEM((widths, HALF), jnp.float32),
            pltpu.SemaphoreType.DMA,
        ],
        cost_estimate=cost(1_000_000_000),
        compiler_params=params(4),
        name="finish",
    )(*operands)


def on_device(snapshots, coeffs):
    axes = ("snap", "param")
    groups = lax.axis_size("snap")
    devices = lax.axis_size(axes)
    total_rows = snapshots.shape[1]
    up_pairs = [(i, (i + 1) % groups) for i in range(groups)]
    down_pairs = [(i, (i - 1) % groups) for i in range(groups)]

    starts = [sum(PARTS[:k]) for k in range(len(PARTS))]

    def both_ways(up, down):
        up = lax.ppermute(up, "snap", up_pairs)
        down = lax.ppermute(down, "snap", down_pairs)
        return up, down

    first, parts, wide = [], [], None
    for start, rows in zip(starts, PARTS):
        up, down, part, *made = sent_sums(snapshots, start, rows, coeffs, wide)
        parts.append(part)
        wide = made[0] if made else wide
        first.append(both_ways(up, down))
    kept = kept_sums(wide, parts)
    second = []
    for start, rows, got in zip(starts, PARTS, first):
        up, down, summed = relay(start, rows, *got, *kept)
        second.append((*both_ways(up, down), summed))
    averages = squares = None
    for start, rows, got in zip(starts, PARTS, second):
        last = start + rows == total_rows
        averages, squares = finish(start, rows, total_rows, devices, last, *got, squares, averages)
    theirs = lax.all_to_all(squares, axes, 0, 0, tiled=True)
    entries = averages.shape[1] * averages.shape[2] * devices
    width_norms = jnp.sqrt(jnp.sum(theirs, axis=0) / jnp.float32(entries))
    return (averages, width_norms)


def solution(mesh):
    return jax.shard_map(
        on_device,
        mesh=mesh,
        in_specs=(P("snap", "param", None), P(None, "snap")),
        out_specs=(P(None, "param", "snap"), P()),
        check_vma=False,
    )
```

```python
import functools

import jax
import jax.numpy as jnp
from jax import lax
from jax.experimental import pallas as pl
from jax.experimental.pallas import tpu as pltpu
from jax.sharding import PartitionSpec as P


GROUP = 8
BLOCK = 16
FLIGHT = 2
HALF = 128
CHUNK = 256
PARTS = (16, 32, 16)

SPAN = 250.0
LN2 = 0.6931471805599453
PRE = 2.0**-8


def column_scale(values):
    top = jnp.max(jnp.abs(values), axis=0, keepdims=True)
    scale = jnp.clip(top * 1.0079, 2.0**-116, 3.38e38)
    return scale.astype(jnp.bfloat16).astype(jnp.float32)


def encode(values, scale):
    inverse = (SPAN * LN2 * PRE) / (scale * PRE)
    code = jnp.exp(jnp.abs(values) * inverse - (SPAN / 2 * LN2))
    return jnp.where(values < 0, -code, code).astype(jnp.bfloat16)


def decode(code, scale):
    code = code.astype(jnp.float32)
    level = jnp.log(jnp.abs(code)) + (SPAN / 2 * LN2)
    return jnp.where(code < 0, -level, level) * (scale * (1.0 / (SPAN * LN2)))


def fill_wide(c_ref, cbuf, sem, wide):
    widths, snaps = c_ref.shape
    depth = snaps * GROUP
    pltpu.make_async_copy(c_ref, cbuf, sem).wait()
    coeffs = cbuf[...]
    high = coeffs.astype(jnp.bfloat16)
    low = (coeffs - high.astype(jnp.float32)).astype(jnp.bfloat16)
    spread = (
        lax.shift_right_logical(lax.broadcasted_iota(jnp.int32, (snaps, depth), 1), 3)
        == lax.broadcasted_iota(jnp.int32, (snaps, depth), 0)
    ).astype(jnp.float32).astype(jnp.bfloat16)
    keep = (lax.broadcasted_iota(jnp.int32, (GROUP, depth), 1) & (GROUP - 1)) == lax.broadcasted_iota(
        jnp.int32, (GROUP, depth), 0
    )
    for part, piece in enumerate((high, low)):
        across = jnp.dot(piece, spread, preferred_element_type=jnp.float32)
        for w in range(widths):
            row = (part * widths + w) * GROUP
            wide[row : row + GROUP, :] = jnp.where(keep, across[w : w + 1, :], 0.0).astype(jnp.bfloat16)


def side():
    return lax.rem(lax.axis_index("snap"), 2)


def half_of(offset):
    return pl.multiple_of(lax.rem(2 * lax.axis_index("snap") + offset, 8) * HALF, HALF)


def multiply(x_ref, wide, start, offsets):
    depth = wide.shape[1]
    half = wide.shape[0] // 2
    halves = [x_ref[:, start : start + GROUP, pl.ds(half_of(offset), HALF)].reshape(depth, HALF) for offset in offsets]
    both = jnp.dot(wide[...], jnp.concatenate(halves, axis=1), preferred_element_type=jnp.float32)
    return (both[:half] + both[half:]).reshape(half // GROUP, GROUP, CHUNK)


def sent_kernel(start, rows, first, x_ref, c_ref, *refs):
    if first:
        up_ref, down_ref, x_out, wide, cbuf, csem, hold, scales, sems = refs
        pltpu.make_async_copy(c_ref, cbuf, csem).start()
    else:
        wide = c_ref
        up_ref, down_ref, x_out, hold, scales, sems = refs
    widths = wide.shape[0] // (2 * GROUP)
    blocks = rows // BLOCK
    copies = [
        pltpu.make_async_copy(
            x_ref.at[:, pl.ds(start + block * BLOCK, BLOCK), :],
            x_out.at[:, pl.ds(block * BLOCK, BLOCK), :],
            sems.at[block],
        )
        for block in range(blocks)
    ]
    for copy in copies[:FLIGHT]:
        copy.start()
    if first:
        fill_wide(c_ref, cbuf, csem, wide)
    p = side() if first else 0
    for block in range(blocks):
        copies[block].wait()
        if block + FLIGHT < blocks:
            copies[block + FLIGHT].start()
        for at in range(block * BLOCK, (block + 1) * BLOCK, GROUP):
            hold[:, at : at + GROUP, :CHUNK] = multiply(x_out, wide, at, (4 + p, 3 + 3 * p))
            hold[:, at : at + GROUP, CHUNK:] = multiply(x_out, wide, at, (5 - p, 6 - 3 * p))
    for w in range(widths):
        value = hold[w]
        scale = column_scale(value)
        scales[w : w + 1, :] = scale
        code = encode(value, scale)
        up_ref[w * rows : (w + 1) * rows, :] = code[:, :CHUNK]
        down_ref[w * rows : (w + 1) * rows, :] = code[:, CHUNK:]
    packed = scales[...].astype(jnp.bfloat16)
    up_ref[widths * rows :, :] = packed[:, :CHUNK]
    down_ref[widths * rows :, :] = packed[:, CHUNK:]


def kept_kernel(wide, *refs):
    x_refs, (own_ref, fwd_up_ref, fwd_down_ref) = refs[:-3], refs[-3:]
    start = 0
    for x_ref in x_refs:
        for at in range(0, x_ref.shape[1], GROUP):
            r = slice(start + at, start + at + GROUP)
            own_ref[:, r, :] = multiply(x_ref, wide, at, (0, 1))
            value = multiply(x_ref, wide, at, (2, 7))
            fwd_up_ref[:, r, :] = value[:, :, :HALF]
            fwd_down_ref[:, r, :] = value[:, :, HALF:]
        start += x_ref.shape[1]


def relay_kernel(start, rows, pairwise, prev_ref, next_ref, own_ref, fwd_up_ref, fwd_down_ref, up_ref, down_ref, sum_ref, scales):
    widths = own_ref.shape[0]
    t = slice(start, start + rows)
    swap = side() == 0
    prev_scale = prev_ref[widths * rows :, :].astype(jnp.float32)
    next_scale = next_ref[widths * rows :, :].astype(jnp.float32)
    for w in range(widths):
        r = slice(w * rows, (w + 1) * rows)
        got_prev = decode(prev_ref[r, :], prev_scale[w : w + 1, :])
        got_next = decode(next_ref[r, :], next_scale[w : w + 1, :])
        if pairwise:
            got_prev, got_next = jnp.where(swap, got_next, got_prev), jnp.where(swap, got_prev, got_next)
        up = fwd_up_ref[w, t, :] + got_prev[:, :HALF]
        down = fwd_down_ref[w, t, :] + got_next[:, :HALF]
        up_scale = column_scale(up)
        down_scale = column_scale(down)
        scales[w : w + 1, :HALF] = up_scale
        scales[w : w + 1, HALF:] = down_scale
        up_ref[r, :] = encode(up, up_scale)
        down_ref[r, :] = encode(down, down_scale)
        sum_ref[w, :, :HALF] = own_ref[w, t, :HALF] + got_next[:, HALF:]
        sum_ref[w, :, HALF:] = own_ref[w, t, HALF:] + got_prev[:, HALF:]
    packed = scales[...].astype(jnp.bfloat16)
    up_ref[widths * rows :, :] = packed[:, :HALF]
    down_ref[widths * rows :, :] = packed[:, HALF:]


def final_kernel(start, rows, first, last, prev_ref, next_ref, sum_ref, *refs):
    refs = list(refs)
    before_ref = None if first else refs.pop(0)
    if not first:
        refs.pop(0)
    out_ref, squares_ref, block, total, sem = refs
    widths = sum_ref.shape[0]
    prev_scale = prev_ref[widths * rows :, :].astype(jnp.float32)
    next_scale = next_ref[widths * rows :, :].astype(jnp.float32)
    for w in range(widths):
        r = slice(w * rows, (w + 1) * rows)
        left = sum_ref[w, :, :HALF] + decode(prev_ref[r, :], prev_scale[w : w + 1, :])
        right = sum_ref[w, :, HALF:] + decode(next_ref[r, :], next_scale[w : w + 1, :])
        block[w, :, :HALF] = left
        block[w, :, HALF:] = right
        total[w : w + 1, :] = jnp.sum(left * left + right * right, axis=0, keepdims=True)
    copy = pltpu.make_async_copy(block, out_ref.at[:, pl.ds(start, rows), :], sem)
    copy.start()
    squares = total[...] if first else total[...] + before_ref[...]
    if last:
        squares = lax.dot_general(
            jnp.ones((squares_ref.shape[0], HALF), jnp.float32),
            squares,
            (((1,), (1,)), ((), ())),
            precision=lax.Precision.HIGHEST,
            preferred_element_type=jnp.float32,
        )
    squares_ref[...] = squares
    copy.wait()


def vmem():
    return pl.BlockSpec(memory_space=pltpu.VMEM)


def hbm():
    return pl.BlockSpec(memory_space=pl.ANY)


def held(array):
    return pltpu.with_memory_space_constraint(array, pltpu.VMEM)


def placed(array):
    return pltpu.with_memory_space_constraint(array, pltpu.HBM)


def cost(flops):
    return pl.CostEstimate(flops=flops, bytes_accessed=2_000_000, transcendentals=0)


def params(mib):
    return pltpu.CompilerParams(vmem_limit_bytes=mib * 2**20)


def sent_sums(snapshots, start, rows, coeffs=None, wide=None):
    first = wide is None
    snaps, _, columns = snapshots.shape
    widths = coeffs.shape[0] if first else wide.shape[0] // (2 * GROUP)
    tall = widths * rows + widths
    wide_shape = pltpu.VMEM((2 * widths * GROUP, snaps * GROUP), jnp.bfloat16)
    return pl.pallas_call(
        functools.partial(sent_kernel, start, rows, first),
        in_specs=[hbm(), hbm() if first else vmem()],
        out_specs=[vmem()] * (4 if first else 3),
        out_shape=[pltpu.VMEM((tall, CHUNK), jnp.bfloat16)] * 2
        + [pltpu.VMEM((snaps, rows, columns), jnp.bfloat16)]
        + [wide_shape] * first,
        scratch_shapes=[pltpu.VMEM((widths, snaps), jnp.float32), pltpu.SemaphoreType.DMA] * first
        + [
            pltpu.VMEM((widths, rows, 2 * CHUNK), jnp.float32),
            pltpu.VMEM((widths, 2 * CHUNK), jnp.float32),
            pltpu.SemaphoreType.DMA((rows // BLOCK,)),
        ],
        cost_estimate=cost(4_000_000_000),
        compiler_params=params(14),
        name="sent_sums",
    )(placed(snapshots), placed(coeffs) if first else held(wide))


def kept_sums(wide, parts):
    widths = wide.shape[0] // (2 * GROUP)
    rows = sum(part.shape[1] for part in parts)
    return pl.pallas_call(
        kept_kernel,
        in_specs=[vmem()] * (1 + len(parts)),
        out_specs=[vmem()] * 3,
        out_shape=[
            pltpu.VMEM((widths, rows, CHUNK), jnp.float32),
            pltpu.VMEM((widths, rows, HALF), jnp.float32),
            pltpu.VMEM((widths, rows, HALF), jnp.float32),
        ],
        cost_estimate=cost(6_000_000_000),
        compiler_params=params(16),
        name="kept_sums",
    )(held(wide), *[held(part) for part in parts])


def relay(start, rows, got_prev, got_next, own, fwd_up, fwd_down):
    widths = own.shape[0]
    tall = widths * rows + widths
    return pl.pallas_call(
        functools.partial(relay_kernel, start, rows, start == 0),
        in_specs=[vmem()] * 5,
        out_specs=[vmem()] * 3,
        out_shape=[
            pltpu.VMEM((tall, HALF), jnp.bfloat16),
            pltpu.VMEM((tall, HALF), jnp.bfloat16),
            pltpu.VMEM((widths, rows, CHUNK), jnp.float32),
        ],
        scratch_shapes=[pltpu.VMEM((widths, CHUNK), jnp.float32)],
        cost_estimate=cost(2_000_000_000),
        compiler_params=params(4),
        name="relay",
    )(held(got_prev), held(got_next), held(own), held(fwd_up), held(fwd_down))


def finish(start, rows, total_rows, devices, last, got_prev, got_next, summed, squares, averages):
    widths = summed.shape[0]
    first = averages is None
    operands = [held(got_prev), held(got_next), held(summed)]
    specs = [vmem()] * 3
    if not first:
        operands += [held(squares), averages]
        specs += [vmem(), hbm()]
    return pl.pallas_call(
        functools.partial(final_kernel, start, rows, first, last),
        in_specs=specs,
        out_specs=[hbm(), vmem()],
        out_shape=[
            jax.ShapeDtypeStruct((widths, total_rows, CHUNK), jnp.float32),
            pltpu.VMEM((devices, widths) if last else (widths, HALF), jnp.float32),
        ],
        input_output_aliases={} if first else {4: 0},
        scratch_shapes=[
            pltpu.VMEM((widths, rows, CHUNK), jnp.float32),
            pltpu.VMEM((widths, HALF), jnp.float32),
            pltpu.SemaphoreType.DMA,
        ],
        cost_estimate=cost(1_000_000_000),
        compiler_params=params(4),
        name="finish",
    )(*operands)


def on_device(snapshots, coeffs):
    axes = ("snap", "param")
    groups = lax.axis_size("snap")
    devices = lax.axis_size(axes)
    total_rows = snapshots.shape[1]
    up_pairs = [(i, (i + 1) % groups) for i in range(groups)]
    down_pairs = [(i, (i - 1) % groups) for i in range(groups)]

    pairs = (
        [(i, (i + 1 - 2 * (i % 2)) % groups) for i in range(groups)],
        [(i, (i - 1 + 2 * (i % 2)) % groups) for i in range(groups)],
    )
    starts = [sum(PARTS[:k]) for k in range(len(PARTS))]

    def both_ways(up, down, up_pairs=up_pairs, down_pairs=down_pairs):
        up = lax.ppermute(up, "snap", up_pairs)
        down = lax.ppermute(down, "snap", down_pairs)
        return up, down

    first, parts, wide = [], [], None
    for k, (start, rows) in enumerate(zip(starts, PARTS)):
        up, down, part, *made = sent_sums(snapshots, start, rows, coeffs, wide)
        parts.append(part)
        wide = made[0] if made else wide
        first.append(both_ways(up, down, *(pairs if k == 0 else ())))
    kept = kept_sums(wide, parts)
    second = []
    for start, rows, got in zip(starts, PARTS, first):
        up, down, summed = relay(start, rows, *got, *kept)
        second.append((*both_ways(up, down), summed))
    averages = squares = None
    for start, rows, got in zip(starts, PARTS, second):
        last = start + rows == total_rows
        averages, squares = finish(start, rows, total_rows, devices, last, *got, squares, averages)
    theirs = lax.all_to_all(squares, axes, 0, 0, tiled=True)
    entries = averages.shape[1] * averages.shape[2] * devices
    width_norms = jnp.sqrt(jnp.sum(theirs, axis=0) / jnp.float32(entries))
    return (averages, width_norms)


def solution(mesh):
    return jax.shard_map(
        on_device,
        mesh=mesh,
        in_specs=(P("snap", "param", None), P(None, "snap")),
        out_specs=(P(None, "param", "snap"), P()),
        check_vma=False,
    )
```
